32 devices in a mesh: row: 4 (over y, x), col: 2 (over core), layer: 4 (over z).
Axes of the slice: x: 2, y: 2, z: 4, core: 2. Of those that a mesh axis runs over, the one named last changes fastest.
Arguments:
- matrix: float32 [4096, 4096], P('row', 'col'), may hold values from -6 to 6
- pattern: int32 [128, 128], P('row', 'col'), may hold values 0 or 1
- keep: int32 [128, 128], P('row', 'col'), may hold values 0 or 1
Outputs:
- update: float32 [4096, 4096], P(('row', 'layer'), 'col')
The draws below stay inside these ranges and needn't reach their ends.
All inputs are finite; a program needn't handle non-finite values. No bound on the sum of `pattern` or of `keep` on one device may be relied on, other than what follows from the above.
Results may differ from the reference program's by a relative error of at most 0.00005.
Values sent between devices are 32-bit elements; how exact they have to be, the bound alone decides.
A program may use at most 128 MiB of HBM per device.

```python
import jax
import jax.numpy as jnp
from jax import lax

BS = 32
NB = 128
ORDER = 4096


def plant(entries, key, low, largest):
    longest = entries.shape.index(max(entries.shape))
    spots = []
    for shift in (0, 1):
        where = [jax.random.randint(jax.random.fold_in(key, axis), (), 0, length) for axis, length in enumerate(entries.shape)]
        where[longest] = (where[longest] + shift) % entries.shape[longest]
        spots.append(tuple(where))
    return entries.at[spots[0]].set(low).at[spots[1]].set(largest)


def shard_levels(rng, dims, shards, low, largest):
    def one(axis_at, blocks):
        steps = jax.random.uniform(jax.random.fold_in(jax.random.fold_in(rng, 6), axis_at), (blocks,), jnp.float32, low / len(shards), largest / len(shards))
        return jnp.repeat(jnp.exp(steps), dims[axis_at] // blocks).reshape((-1,) + (1,) * (len(dims) - axis_at - 1))

    gain = one(*shards[0])
    for cut in shards[1:]:
        gain = gain * one(*cut)
    return gain


def normal_values(key, shape, deviation, limit, shards=(), kind=jnp.bfloat16):
    entries = deviation * jax.random.normal(key, shape, jnp.float32)
    if shards:
        entries = entries * shard_levels(key, shape, shards, -0.22, 0.18)
    return jnp.clip(entries, -limit, limit).astype(kind)


def setup_inputs(seed: int = 0) -> dict:
    streams_of = jax.random.split(jax.random.key(seed), 4)
    return {
        "matrix": normal_values(streams_of[0], (ORDER, ORDER), 1.0, 6.0, ((0, 4), (1, 2)), jnp.float32),
        "pattern": plant((jax.random.randint(streams_of[1], (NB, NB), 0, 2) < 1).astype(jnp.int32), jax.random.fold_in(streams_of[1], 1), 0, 1),
        "keep": plant((jax.random.randint(streams_of[2], (NB, NB), 0, 4) < 3).astype(jnp.int32), jax.random.fold_in(streams_of[2], 1), 0, 1),
    }


def blockwise(values, flags):
    shaped = values.reshape(NB, BS, NB, BS) * flags.astype(jnp.float32)[:, None, :, None]
    return shaped.reshape(NB * BS, NB * BS)


def reference(matrix, pattern, keep):
    sparse = blockwise(matrix, pattern)
    square = jnp.dot(sparse, sparse, preferred_element_type=jnp.float32, precision=lax.Precision.HIGHEST)
    filtered = blockwise(square, keep)
    product = jnp.dot(sparse, filtered, preferred_element_type=jnp.float32, precision=lax.Precision.HIGHEST)
    factor = 0.72 / (NB * BS)
    return 1.5 * sparse - (0.5 * factor) * product
```

```python
import jax
import jax.numpy as jnp
from jax import lax
from jax.sharding import PartitionSpec as P

BS = 32
NB = 128


def layer_rows(values, layers, level):
    count, width = values.shape
    shaped = values.reshape(count // (layers * BS), layers, BS, width)
    picked = lax.dynamic_index_in_dim(shaped, level, 1, keepdims=False)
    return picked.reshape(count // layers, width)


def local(matrix, pattern, keep):
    rows, cols = matrix.shape
    block_rows, block_cols = pattern.shape
    layers = lax.axis_size("layer")
    level = lax.axis_index("layer")
    sparse = (
        matrix.reshape(block_rows, BS, block_cols, BS)
        * pattern.astype(jnp.float32)[:, None, :, None]
    ).reshape(rows, cols)
    left_local = lax.dynamic_index_in_dim(
        sparse.reshape(rows, block_cols // layers, layers, BS), level, 2, keepdims=False
    )
    left_local = left_local.reshape(rows, block_cols // layers * BS)
    left_full = lax.all_gather(left_local, "col", axis=1, tiled=True)
    right_full = lax.all_gather(layer_rows(sparse, layers, level), "row", axis=0, tiled=True)
    partial_value = jnp.dot(
        left_full, right_full, preferred_element_type=jnp.float32, precision=lax.Precision.HIGH
    )
    keep_flags = keep.astype(jnp.float32)
    keep_mine = lax.dynamic_index_in_dim(
        keep_flags.reshape(block_rows // layers, layers, block_cols), level, 1, keepdims=False
    )
    by_layer = partial_value.reshape(block_rows // layers, layers, BS, cols).transpose(1, 0, 2, 3)
    mine = lax.psum_scatter(
        by_layer.reshape(rows, cols), "layer", scatter_dimension=0, tiled=True
    )
    filtered = (
        mine.reshape(block_rows // layers, BS, block_cols, BS) * keep_mine[:, None, :, None]
    ).reshape(rows // layers, cols)
    filtered_full = lax.all_gather(filtered, "row", axis=0, tiled=True)
    share = rows // layers
    summed = lax.psum_scatter(
        jnp.dot(
            left_full,
            filtered_full,
            preferred_element_type=jnp.float32,
            precision=lax.Precision.HIGH,
        ),
        "layer",
        scatter_dimension=0,
        tiled=True,
    )
    own_rows = lax.dynamic_slice_in_dim(sparse, level * share, share, 0)
    factor = 0.72 / (NB * BS)
    return 1.5 * own_rows - 0.5 * factor * summed


def solution(mesh):
    placed = (P("row", "col"), P("row", "col"), P("row", "col"))
    return jax.shard_map(
        local, mesh=mesh, in_specs=placed, out_specs=P(("row", "layer"), "col"), check_vma=False
    )
```
